32 devices in a mesh: rep: 4 (over z), tok: 4 (over x, core), voc: 2 (over y).
Axes of the slice: x: 2, y: 2, z: 4, core: 2. Of those that a mesh axis runs over, the one named last changes fastest.
Arguments:
- hidden: bfloat16 [4, 64, 4096], P('rep', ('tok', 'voc')), may hold values from -500 to 500
- targets: int32 [4, 64], P('rep', ('tok', 'voc')), may hold values from 0 to 8191
- unembed: bfloat16 [4, 8192, 4096], P('rep', ('tok', 'voc')), may hold values from -1 to 1
- outer_weight: float32 [1024, 4096], P(('tok', 'voc'), 'rep'), may hold values from -0.9 to 0.9
- momentum: float32 [1024, 4096], P(('tok', 'voc'), 'rep'), may hold values from -0.18 to 0.18
Outputs:
- token_loss: float32 [4, 64], P('rep', ('tok', 'voc'))
- hidden_grad: float32 [4, 64, 4096], P('rep', ('tok', 'voc'))
- new_outer: float32 [1024, 4096], P(('tok', 'voc'), 'rep')
- new_momentum: float32 [1024, 4096], P(('tok', 'voc'), 'rep')
- next_inner: bfloat16 [1024, 4096], P(('tok', 'voc'))
The draws below stay inside these ranges and needn't reach their ends.
All inputs are finite; a program needn't handle non-finite values.
Results may differ from the reference program's by a relative error of at most 0.0085.
Values may be sent and summed in bfloat16 or wider, within the bound.
A program may use at most 64 MiB of HBM per device.

```python
import math
import jax
import jax.numpy as jnp
import numpy as np
from jax import lax

D = 4096
VOC_DEV = 1024
SLAB_DEV = 128
REPLICAS = 4
TOKENS = 64
VOCAB = 8192
SLAB = 1024


weight_scale = 0.15


state_scale = 20.0


def base_rows(key, row_ids):
    base_key = jax.random.fold_in(key, 101)

    def one_row(row):
        noise = jax.random.normal(jax.random.fold_in(base_key, row), (D,), jnp.float32)
        return weight_scale * jnp.clip(noise, -6.0, 6.0)
    return jax.vmap(one_row)(row_ids)


def inner_rows(key, replica, row_ids):
    drift_key = jax.random.fold_in(key, 202)

    def one_row(row):
        noise = jax.random.normal(jax.random.fold_in(drift_key, replica * VOCAB + row), (D,), jnp.float32)
        return 0.1 * weight_scale * jnp.clip(noise, -6.0, 6.0)
    return base_rows(key, row_ids) + jax.vmap(one_row)(row_ids)


def draw_unembed(key, part):
    row_ids = jnp.arange(VOCAB, dtype=jnp.int32)

    def one_replica(replica):
        return inner_rows(key, replica, row_ids).astype(jnp.bfloat16)
    return lax.map(one_replica, jnp.arange(REPLICAS, dtype=jnp.int32))


def draw_outer_weight(key, part):
    slab_index = jnp.arange(SLAB, dtype=jnp.int32)
    row_ids = slab_index // SLAB_DEV * VOC_DEV + slab_index % SLAB_DEV
    return base_rows(key, row_ids)


def draw_hidden(key, part):
    noise = jnp.clip(jax.random.normal(jax.random.fold_in(key, 303), (REPLICAS, TOKENS, D), jnp.float32), -6.0, 6.0)
    return (state_scale * noise).astype(jnp.bfloat16)


def place_ends(drawn, rng, least, high):
    shape = drawn.shape
    spot = [jax.random.randint(jax.random.fold_in(rng, axis), (), 0, shape[axis]) for axis in range(len(shape))]
    drawn = drawn.at[tuple(spot)].set(least)
    longest = shape.index(max(shape))
    spot[longest] = (spot[longest] + 1) % shape[longest]
    return drawn.at[tuple(spot)].set(high)


def block_levels(stream_key, dims, split, low, high):
    loudness = 1.0
    for position, blocks in split:
        steps = jax.random.uniform(jax.random.fold_in(jax.random.fold_in(stream_key, 6), position), (blocks,), jnp.float32, low / len(split), high / len(split))
        loudness = loudness * jnp.repeat(jnp.exp(steps), dims[position] // blocks).reshape((-1,) + (1,) * (len(dims) - 1 - position))
    return loudness


def rank_table(number_of, lean):
    weights = [(1 << 20) // math.isqrt(grade ** lean) + 1 for grade in range(1, number_of + 1)]
    spread = 1 + sum(weights) // (1 << 30)
    return np.cumsum(np.array([max(1, weight // spread) for weight in weights]))


def skewed_ids(own_key, shape, count, lean):
    table = rank_table(count, lean)
    pick = jax.random.randint(jax.random.fold_in(own_key, 1), shape, 0, int(table[count - 1]))
    standing = jnp.searchsorted(jnp.asarray(table, jnp.int32), pick, side="right")
    return jax.random.permutation(jax.random.fold_in(own_key, 2), count)[standing].astype(jnp.int32)


def centred(rng, shape, deviation, bound, shards=(), held_as=jnp.bfloat16):
    gain = block_levels(rng, shape, shards, -0.22, 0.18) if shards else 1.0
    array = jax.random.normal(rng, shape, jnp.float32) * deviation * gain
    return jnp.minimum(jnp.maximum(array, -bound), bound).astype(held_as)


def setup_inputs(seed: int = 0) -> dict:
    splits = jax.random.split(jax.random.key(seed), 6)
    hidden = draw_hidden(jax.random.fold_in(splits[5], 71), 0)
    targets = place_ends(skewed_ids(splits[1], (REPLICAS, TOKENS), VOCAB, 2), jax.random.fold_in(splits[1], 3), 0, VOCAB - 1).astype(jnp.int32)
    unembed = draw_unembed(jax.random.fold_in(splits[5], 71), 0)
    outer_weight = draw_outer_weight(jax.random.fold_in(splits[5], 71), 0)
    momentum = centred(splits[4], (SLAB, D), 0.03, 0.18, ((0, 8), (1, 4)), jnp.float32)
    return {"hidden": hidden, "targets": targets, "unembed": unembed, "outer_weight": outer_weight, "momentum": momentum}


inner_rate = 0.5
outer_rate = 0.7
momentum_coef = 0.9


def replica_step(inputs):
    states, labels, weights = inputs
    model_width = states.shape[1]
    logit_scale = model_width ** -0.5
    vocab_size = weights.shape[0]
    logits = jnp.dot(states, weights.T, preferred_element_type=jnp.float32) * logit_scale
    row_top = jnp.max(logits, axis=1)
    log_total = row_top + jnp.log(jnp.sum(jnp.exp(logits - row_top[:, None]), axis=1))
    onehot = labels[:, None] == jnp.arange(vocab_size, dtype=jnp.int32)[None, :]
    target_logit = jnp.sum(jnp.where(onehot, logits, 0.0), axis=1)
    token_loss = log_total - target_logit
    errors = (jnp.exp(logits - log_total[:, None]) - onehot.astype(jnp.float32)).astype(jnp.bfloat16)
    hidden_grad = jnp.dot(errors, weights, preferred_element_type=jnp.float32) * logit_scale
    slab_index = jnp.arange(SLAB, dtype=jnp.int32)
    slab_rows = (slab_index // SLAB_DEV) * VOC_DEV + slab_index % SLAB_DEV
    slab_errors = jnp.take(errors, slab_rows, axis=1)
    slab_grad = jnp.dot(slab_errors.T, states, preferred_element_type=jnp.float32) * logit_scale
    final_slab = jnp.take(weights, slab_rows, axis=0).astype(jnp.float32) - inner_rate * slab_grad
    return token_loss, hidden_grad, final_slab


def reference(hidden, targets, unembed, outer_weight, momentum):
    token_loss, hidden_grad, final_slab = lax.map(replica_step, (hidden, targets, unembed))
    mean_final = jnp.mean(final_slab, axis=0)
    pseudo_grad = outer_weight - mean_final
    new_momentum = momentum_coef * momentum + pseudo_grad
    new_outer = outer_weight - outer_rate * (pseudo_grad + momentum_coef * new_momentum)
    next_inner = new_outer.astype(jnp.bfloat16)
    return token_loss, hidden_grad, new_outer, new_momentum, next_inner
```

```python
import functools

import jax
import jax.numpy as jnp
from jax import lax
from jax.experimental import pallas as pl
from jax.experimental.pallas import tpu as pltpu
from jax.sharding import PartitionSpec as P

inner_rate = 0.5
outer_rate = 0.7
momentum_coef = 0.9
F32 = jnp.float32
BF16 = jnp.bfloat16


def kernel(
    sizes,
    hid, tgt, w_hbm, outer_hbm, mom_hbm,
    loss_out, grad_out, outer_out, mom_out, next_out,
    w, hbuf, h2d, tbuf, hz, wz, logits, errs, ez, stat, gsend, grecv, outer_v, mom_v, nsend,
    wsem, lsem, hs, hr, ts, tr, zhs, zhr, zws, zwr, hzs, hzr, ss, sr, es, er, gs, gr, ns, nr,
):
    R, T, V, rows, D, vocab, slab, feat, wch, gch = sizes
    n = T * V
    tokens = n * rows
    scale = D ** -0.5
    rep = lax.axis_index("rep")
    g = lax.axis_index("tok") * V + lax.axis_index("voc")

    def group_id(p):
        return {"tok": p // V, "voc": lax.rem(p, V)}

    def over_group(body):
        def step(d, c):
            body(d, lax.rem(g + d, n))
            return c
        lax.fori_loop(1, n, step, 0)

    def over_reps(body):
        for d in range(1, R):
            body(d, lax.rem(rep + d, R))

    def feats(p):
        return pl.ds(pl.multiple_of(p * feat, feat), feat)

    hid_in = pltpu.make_async_copy(hid, hbuf.at[g], lsem.at[0])
    hid_in.start()
    hz_in = pltpu.make_async_copy(hid.at[:, feats(rep)], hz.at[g, rep], lsem.at[1])
    hz_in.start()
    w_in = lambda c: pltpu.make_async_copy(
        w_hbm.at[pl.ds(pl.multiple_of(c * wch, wch), wch)],
        w.at[pl.ds(pl.multiple_of(c * wch, wch), wch)], wsem.at[c])
    for c in range(vocab // wch):
        w_in(c).start()
    outer_in = pltpu.make_async_copy(outer_hbm, outer_v, lsem.at[2])
    outer_in.start()
    mom_in = pltpu.make_async_copy(mom_hbm, mom_v, lsem.at[3])
    mom_in.start()

    diag = lax.broadcasted_iota(jnp.int32, (rows, rows), 0) == lax.broadcasted_iota(jnp.int32, (rows, rows), 1)
    trow = jnp.broadcast_to(tgt[...].astype(F32), (rows, rows))
    tcol = jnp.sum(jnp.where(diag, trow, 0.0), axis=1, keepdims=True)
    tbuf[g] = jnp.broadcast_to(tcol, (rows, 128))

    barrier = pltpu.get_barrier_semaphore()
    over_reps(lambda d, p: pl.semaphore_signal(barrier, inc=1, device_id={"rep": p}))
    over_group(lambda d, p: pl.semaphore_signal(barrier, inc=1, device_id=group_id(p)))
    pl.semaphore_wait(barrier, R - 1 + n - 1)

    def zh(d, p, s):
        return pltpu.make_async_remote_copy(
            hid.at[:, feats(p)], hz.at[g, rep if s else p], zhs.at[d], zhr.at[rep if s else p], device_id={"rep": p})

    def zw(d, p, s):
        return pltpu.make_async_remote_copy(
            w_hbm.at[pl.ds(0, slab), feats(p)], wz.at[rep if s else p], zws.at[d], zwr.at[rep if s else p],
            device_id={"rep": p})

    over_reps(lambda d, p: zh(d, p, True).start())
    hid_in.wait()

    def hx(d, p, s):
        o = g if s else p
        return pltpu.make_async_remote_copy(hbuf.at[g], hbuf.at[o], hs.at[d], hr.at[o], device_id=group_id(p))

    def tx(d, p, s):
        o = g if s else p
        return pltpu.make_async_remote_copy(tbuf.at[g], tbuf.at[o], ts.at[d], tr.at[o], device_id=group_id(p))

    def start_group(d, p):
        hx(d, p, True).start()
        tx(d, p, True).start()
    over_group(start_group)
    over_reps(lambda d, p: zw(d, p, True).start())

    def wait_group(d, p):
        hx(d, p, False).wait_recv()
    over_group(wait_group)

    def pack(i, c):
        cols = pl.ds(pl.multiple_of(i * gch, gch), gch)
        h2d[:, cols] = hbuf[:, :, cols].astype(F32).reshape(tokens, gch).astype(BF16)
        return c
    lax.fori_loop(0, D // gch, pack, 0)

    def logit_step(c, carry):
        w_in(c).wait()
        at = pl.ds(pl.multiple_of(c * wch, wch), wch)
        logits[:, at] = lax.dot_general(
            h2d[...], w[at], (((1,), (1,)), ((), ())), preferred_element_type=F32) * scale
        return carry
    lax.fori_loop(0, vocab // wch, logit_step, 0)

    hz_in.wait()
    over_reps(lambda d, p: zh(d, p, False).wait_recv())

    def hzx(d, p, s):
        o = g if s else p
        return pltpu.make_async_remote_copy(hz.at[g], hz.at[o], hzs.at[d], hzr.at[o], device_id=group_id(p))

    over_group(lambda d, p: tx(d, p, False).wait_recv())
    l = logits[...]
    targets = tbuf[...].reshape(tokens, 128)[:, :1].astype(jnp.int32)
    onehot = targets == g * vocab + lax.broadcasted_iota(jnp.int32, (tokens, vocab), 1)
    top = jnp.max(l, axis=1, keepdims=True)
    ex = jnp.exp(l - top)
    total = jnp.sum(ex, axis=1, keepdims=True)
    tl = jnp.sum(jnp.where(onehot, l, 0.0), axis=1, keepdims=True)
    lanes = stat.shape[2]
    eye = lax.broadcasted_iota(jnp.int32, (tokens, lanes), 0) == lax.broadcasted_iota(jnp.int32, (tokens, lanes), 1)
    to_row = lambda col: jnp.sum(jnp.where(eye, col, 0.0), axis=0, keepdims=True)
    to_col = lambda row: jnp.sum(jnp.where(eye, row, 0.0), axis=1, keepdims=True)
    stat[g] = jnp.concatenate([to_row(top), to_row(total), to_row(tl), jnp.zeros((5, lanes), F32)], axis=0)

    def sx(d, p, s):
        o = g if s else p
        return pltpu.make_async_remote_copy(stat.at[g], stat.at[o], ss.at[d], sr.at[o], device_id=group_id(p))
    over_group(lambda d, p: sx(d, p, True).start())
    over_group(lambda d, p: hzx(d, p, True).start())
    over_group(lambda d, p: sx(d, p, False).wait_recv())
    st = stat[...]
    tops = st[:, 0:1, :]
    all_top = jnp.max(tops, axis=0)
    all_total = jnp.sum(st[:, 1:2, :] * jnp.exp(tops - all_top[None]), axis=0)
    log_total = all_top + jnp.log(all_total)
    loss_row = log_total - jnp.sum(st[:, 2:3, :], axis=0)
    loss_col = to_col(loss_row)
    mine = lax.broadcasted_iota(jnp.int32, (tokens, rows), 0) == g * rows + lax.broadcasted_iota(
        jnp.int32, (tokens, rows), 1)
    loss_out[...] = jnp.sum(jnp.where(mine, loss_col, 0.0), axis=0, keepdims=True)
    err = (jnp.exp(l - to_col(log_total)) - onehot.astype(F32)).astype(BF16)
    errs[...] = err
    ez[rep] = err[:, :slab]

    def zx(d, p, s):
        o = rep if s else p
        return pltpu.make_async_remote_copy(ez.at[rep], ez.at[o], es.at[d], er.at[o], device_id={"rep": p})
    over_reps(lambda d, p: zx(d, p, True).start())

    def grad_step(i, c):
        cols = pl.ds(pl.multiple_of(i * gch, gch), gch)
        part = jnp.dot(errs[...], w[:, cols], preferred_element_type=F32) * scale
        gsend[:, :, cols] = part.reshape(n, rows, gch).astype(BF16)
        return c
    lax.fori_loop(0, D // gch, grad_step, 0)

    def gx(d, p, s):
        return pltpu.make_async_remote_copy(
            gsend.at[p], grecv.at[g if s else p], gs.at[d], gr.at[g if s else p], device_id=group_id(p))
    over_group(lambda d, p: gx(d, p, True).start())

    over_group(lambda d, p: hzx(d, p, False).wait_recv())
    over_reps(lambda d, p: zx(d, p, False).wait_recv())
    outer_in.wait()
    mom_in.wait()
    every_err = ez[...].astype(F32).reshape(R * tokens, slab).T.astype(BF16)
    every_hid = jnp.concatenate(
        [hz[:, r].astype(F32).reshape(tokens, feat).astype(BF16) for r in range(R)], axis=0)
    slab_grad = jnp.dot(every_err, every_hid, preferred_element_type=F32) * scale
    over_reps(lambda d, p: zw(d, p, False).wait_recv())
    wz[rep] = w[:slab, feats(rep)]
    final_sum = jnp.sum(wz[...].astype(F32), axis=0) - inner_rate * slab_grad
    outer = outer_v[...]
    pseudo = outer - final_sum / R
    moved_mom = momentum_coef * mom_v[...] + pseudo
    moved = outer - outer_rate * (pseudo + momentum_coef * moved_mom)
    mom_out[...] = moved_mom
    outer_out[...] = moved
    low = moved.astype(BF16)
    nsend[...] = low

    def nx(d, p, s):
        return pltpu.make_async_remote_copy(
            nsend, next_out.at[:, feats(rep if s else p)], ns.at[d], nr.at[rep if s else p], device_id={"rep": p})
    over_reps(lambda d, p: nx(d, p, True).start())
    next_out[:, feats(rep)] = low

    over_group(lambda d, p: gx(d, p, False).wait_recv())
    grecv[g] = gsend[g]

    def grad_sum(i, c):
        cols = pl.ds(pl.multiple_of(i * gch, gch), gch)
        grad_out[:, cols] = jnp.sum(grecv[:, :, cols].astype(F32), axis=0)
        return c
    lax.fori_loop(0, D // gch, grad_sum, 0)

    def drain_group(d, p):
        for x in (hx, tx, hzx, sx, gx):
            x(d, p, True).wait_send()
    over_group(drain_group)

    def drain_reps(d, p):
        for x in (zh, zw, zx, nx):
            x(d, p, True).wait_send()
    over_reps(drain_reps)
    over_reps(lambda d, p: nx(d, p, False).wait_recv())


def per_device(hidden, targets, unembed, outer_weight, momentum):
    R, T, V = lax.axis_size("rep"), lax.axis_size("tok"), lax.axis_size("voc")
    n = T * V
    _, rows, D = hidden.shape
    vocab = unembed.shape[1]
    slab, feat = outer_weight.shape
    tokens = n * rows
    lanes = -(-tokens // 128) * 128
    wch = min(256, vocab)
    gch = min(512, D)
    dma = pltpu.SemaphoreType.DMA
    vm = pltpu.VMEM
    spec_v = pl.BlockSpec(memory_space=pltpu.VMEM)
    spec_a = pl.BlockSpec(memory_space=pl.ANY)
    scratch = [
        vm((vocab, D), BF16), vm((n, rows, D), BF16), vm((tokens, D), BF16), vm((n, rows, 128), F32),
        vm((n, R, rows, feat), BF16), vm((R, slab, feat), BF16), vm((tokens, vocab), F32),
        vm((tokens, vocab), BF16), vm((R, tokens, slab), BF16), vm((n, 8, lanes), F32),
        vm((n, rows, D), BF16), vm((n, rows, D), BF16), vm((slab, feat), F32), vm((slab, feat), F32),
        vm((slab, feat), BF16),
        dma((vocab // wch,)), dma((4,)),
        dma((n,)), dma((n,)), dma((n,)), dma((n,)), dma((R,)), dma((R,)), dma((R,)), dma((R,)),
        dma((n,)), dma((n,)), dma((n,)), dma((n,)), dma((R,)), dma((R,)), dma((n,)), dma((n,)), dma((R,)), dma((R,)),
    ]
    loss, grad, new_outer, new_mom, nxt = pl.pallas_call(
        functools.partial(kernel, (R, T, V, rows, D, vocab, slab, feat, wch, gch)),
        out_shape=(
            jax.ShapeDtypeStruct((1, rows), F32),
            jax.ShapeDtypeStruct((rows, D), F32),
            jax.ShapeDtypeStruct((slab, feat), F32),
            jax.ShapeDtypeStruct((slab, feat), F32),
            jax.ShapeDtypeStruct((slab, R * feat), BF16),
        ),
        in_specs=[spec_a, spec_v, spec_a, spec_a, spec_a],
        out_specs=(spec_v,) * 5,
        scratch_shapes=scratch,
        compiler_params=pltpu.CompilerParams(
            collective_id=0, has_side_effects=True, vmem_limit_bytes=60 * 1024 * 1024),
        name="step",
    )(hidden[0], targets, unembed[0], outer_weight, momentum)
    return (loss, grad[None], new_outer, new_mom, nxt)


def solution(mesh):
    group = ("tok", "voc")
    return jax.shard_map(
        per_device,
        mesh=mesh,
        in_specs=(P("rep", group, None), P("rep", group), P("rep", group, None), P(group, "rep"), P(group, "rep")),
        out_specs=(P("rep", group), P("rep", group, None), P(group, "rep"), P(group, "rep"), P(group, None)),
        check_vma=False,
    )
```

```python
import functools

import jax
import jax.numpy as jnp
from jax import lax
from jax.experimental import pallas as pl
from jax.experimental.pallas import tpu as pltpu
from jax.sharding import PartitionSpec as P

inner_rate = 0.5
outer_rate = 0.7
momentum_coef = 0.9
F32 = jnp.float32
BF16 = jnp.bfloat16


def kernel(
    sizes,
    hid, tgt, w_hbm, outer_v, mom_v,
    loss_out, grad_out, outer_out, mom_out, next_out,
    w, hbuf, h2d, tbuf, hz, wz, logits, errs, ez, stat, gsend, grecv, sgrad,
    wsem, lsem, hs, hr, ts, tr, zhs, zhr, zws, zwr, hzs, hzr, ss, sr, es, er, gs, gr, nright, nleft, nr,
):
    R, T, V, rows, D, vocab, slab, feat, wch, gch, parts = sizes
    prow = slab // parts
    n = T * V
    tokens = n * rows
    scale = D ** -0.5
    rep = lax.axis_index("rep")
    g = lax.axis_index("tok") * V + lax.axis_index("voc")

    def group_id(p):
        return {"tok": p // V, "voc": lax.rem(p, V)}

    def over_group(body):
        def step(d, c):
            body(d, lax.rem(g + d, n))
            return c
        lax.fori_loop(1, n, step, 0)

    def over_reps(body):
        for d in range(1, R):
            body(d, lax.rem(rep + d, R))

    def feats(p):
        return pl.ds(pl.multiple_of(p * feat, feat), feat)

    hid_in = pltpu.make_async_copy(hid, hbuf.at[g], lsem.at[0])
    hid_in.start()
    hz_in = pltpu.make_async_copy(hid.at[:, feats(rep)], hz.at[g, rep], lsem.at[1])
    hz_in.start()
    w_in = lambda c: pltpu.make_async_copy(
        w_hbm.at[pl.ds(pl.multiple_of(c * wch, wch), wch)],
        w.at[pl.ds(pl.multiple_of(c * wch, wch), wch)], wsem.at[c])
    for c in range(vocab // wch):
        w_in(c).start()

    diag = lax.broadcasted_iota(jnp.int32, (rows, rows), 0) == lax.broadcasted_iota(jnp.int32, (rows, rows), 1)
    trow = jnp.broadcast_to(tgt[...].astype(F32), (rows, rows))
    tcol = jnp.sum(jnp.where(diag, trow, 0.0), axis=1, keepdims=True)
    tbuf[g] = jnp.broadcast_to(tcol, (rows, 128))

    barrier = pltpu.get_barrier_semaphore()
    over_reps(lambda d, p: pl.semaphore_signal(barrier, inc=1, device_id={"rep": p}))
    over_group(lambda d, p: pl.semaphore_signal(barrier, inc=1, device_id=group_id(p)))
    pl.semaphore_wait(barrier, R - 1 + n - 1)

    def zh(d, p, s):
        return pltpu.make_async_remote_copy(
            hid.at[:, feats(p)], hz.at[g, rep if s else p], zhs.at[d], zhr.at[rep if s else p], device_id={"rep": p})

    def zw(k, d, p, s):
        o = rep if s else p
        return pltpu.make_async_remote_copy(
            w_hbm.at[pl.ds(k * prow, prow), feats(p)], wz.at[o, pl.ds(k * prow, prow)], zws.at[k, d], zwr.at[k, o],
            device_id={"rep": p})

    over_reps(lambda d, p: zh(d, p, True).start())
    hid_in.wait()

    def hx(d, p, s):
        o = g if s else p
        return pltpu.make_async_remote_copy(hbuf.at[g], hbuf.at[o], hs.at[d], hr.at[o], device_id=group_id(p))

    def tx(d, p, s):
        o = g if s else p
        return pltpu.make_async_remote_copy(tbuf.at[g], tbuf.at[o], ts.at[d], tr.at[o], device_id=group_id(p))

    def start_group(d, p):
        hx(d, p, True).start()
        tx(d, p, True).start()
    over_group(start_group)
    for k in range(parts):
        over_reps(lambda d, p: zw(k, d, p, True).start())

    def wait_group(d, p):
        hx(d, p, False).wait_recv()
    over_group(wait_group)

    def pack(i, c):
        cols = pl.ds(pl.multiple_of(i * gch, gch), gch)
        h2d[:, cols] = hbuf[:, :, cols].astype(F32).reshape(tokens, gch).astype(BF16)
        return c
    lax.fori_loop(0, D // gch, pack, 0)

    def logit_step(c, carry):
        w_in(c).wait()
        at = pl.ds(pl.multiple_of(c * wch, wch), wch)
        logits[:, at] = lax.dot_general(
            h2d[...], w[at], (((1,), (1,)), ((), ())), preferred_element_type=F32) * scale
        return carry
    lax.fori_loop(0, vocab // wch, logit_step, 0)

    hz_in.wait()
    over_reps(lambda d, p: zh(d, p, False).wait_recv())

    def hzx(d, p, s):
        o = g if s else p
        return pltpu.make_async_remote_copy(hz.at[g], hz.at[o], hzs.at[d], hzr.at[o], device_id=group_id(p))

    over_group(lambda d, p: tx(d, p, False).wait_recv())
    l = logits[...]
    targets = tbuf[...].reshape(tokens, 128)[:, :1].astype(jnp.int32)
    onehot = targets == g * vocab + lax.broadcasted_iota(jnp.int32, (tokens, vocab), 1)
    top = jnp.max(l, axis=1, keepdims=True)
    ex = jnp.exp(l - top)
    total = jnp.sum(ex, axis=1, keepdims=True)
    tl = jnp.sum(jnp.where(onehot, l, 0.0), axis=1, keepdims=True)
    lanes = stat.shape[2]
    eye = lax.broadcasted_iota(jnp.int32, (tokens, lanes), 0) == lax.broadcasted_iota(jnp.int32, (tokens, lanes), 1)
    to_row = lambda col: jnp.sum(jnp.where(eye, col, 0.0), axis=0, keepdims=True)
    to_col = lambda row: jnp.sum(jnp.where(eye, row, 0.0), axis=1, keepdims=True)
    stat[g] = jnp.concatenate([to_row(top), to_row(total), to_row(tl), jnp.zeros((5, lanes), F32)], axis=0)

    def sx(d, p, s):
        o = g if s else p
        return pltpu.make_async_remote_copy(stat.at[g], stat.at[o], ss.at[d], sr.at[o], device_id=group_id(p))
    over_group(lambda d, p: sx(d, p, True).start())
    over_group(lambda d, p: hzx(d, p, True).start())
    over_group(lambda d, p: sx(d, p, False).wait_recv())
    st = stat[...]
    tops = st[:, 0:1, :]
    all_top = jnp.max(tops, axis=0)
    all_total = jnp.sum(st[:, 1:2, :] * jnp.exp(tops - all_top[None]), axis=0)
    log_total = all_top + jnp.log(all_total)
    loss_row = log_total - jnp.sum(st[:, 2:3, :], axis=0)
    loss_col = to_col(loss_row)
    mine = lax.broadcasted_iota(jnp.int32, (tokens, rows), 0) == g * rows + lax.broadcasted_iota(
        jnp.int32, (tokens, rows), 1)
    loss_out[...] = jnp.sum(jnp.where(mine, loss_col, 0.0), axis=0, keepdims=True)
    err = (jnp.exp(l - to_col(log_total)) - onehot.astype(F32)).astype(BF16)
    errs[...] = err
    ez[rep] = err[:, :slab]

    def zx(d, p, s):
        o = rep if s else p
        return pltpu.make_async_remote_copy(ez.at[rep], ez.at[o], es.at[d], er.at[o], device_id={"rep": p})
    over_reps(lambda d, p: zx(d, p, True).start())

    def grad_step(i, c):
        cols = pl.ds(pl.multiple_of(i * gch, gch), gch)
        part = jnp.dot(errs[...], w[:, cols], preferred_element_type=F32) * scale
        gsend[:, :, cols] = part.reshape(n, rows, gch).astype(BF16)
        return c
    lax.fori_loop(0, D // gch, grad_step, 0)

    def gx(d, p, s):
        return pltpu.make_async_remote_copy(
            gsend.at[p], grecv.at[g if s else p], gs.at[d], gr.at[g if s else p], device_id=group_id(p))
    over_group(lambda d, p: gx(d, p, True).start())

    over_group(lambda d, p: hzx(d, p, False).wait_recv())
    over_reps(lambda d, p: zx(d, p, False).wait_recv())
    every_err = ez[...].astype(F32).reshape(R * tokens, slab).T.astype(BF16)
    every_hid = jnp.concatenate(
        [hz[:, r].astype(F32).reshape(tokens, feat).astype(BF16) for r in range(R)], axis=0)
    sgrad[...] = jnp.dot(every_err, every_hid, preferred_element_type=F32) * scale
    wz[rep] = w[:slab, feats(rep)]

    def nx(k, b, side):
        at = next_out.at[pl.ds(k * prow, prow), feats(b)]
        sems = nright if side > 0 else nleft
        return pltpu.make_async_remote_copy(
            at, at, sems.at[k, b], nr.at[k, b], device_id={"rep": lax.rem(rep + side + R, R)})

    has_right, has_left = rep < R - 1, rep > 0

    def outer_part(k):
        at = pl.ds(k * prow, prow)
        over_reps(lambda d, p: zw(k, d, p, False).wait_recv())
        final_sum = jnp.sum(wz[:, at].astype(F32), axis=0) - inner_rate * sgrad[at]
        outer = outer_v[at]
        pseudo = outer - final_sum / R
        moved_mom = momentum_coef * mom_v[at] + pseudo
        moved = outer - outer_rate * (pseudo + momentum_coef * moved_mom)
        mom_out[at] = moved_mom
        outer_out[at] = moved
        next_out[at, feats(rep)] = moved.astype(BF16)
        pl.when(has_right)(lambda: nx(k, rep, 1).start())
        pl.when(has_left)(lambda: nx(k, rep, -1).start())

    def relay(k):
        for d in range(1, R):
            @pl.when(rep >= d)
            def _():
                nx(k, rep - d, 1).wait_recv()
                pl.when(has_right)(lambda: nx(k, rep - d, 1).start())

            @pl.when(rep + d < R)
            def _():
                nx(k, rep + d, -1).wait_recv()
                pl.when(has_left)(lambda: nx(k, rep + d, -1).start())

    for k in range(parts):
        outer_part(k)
        if k > 0:
            relay(k - 1)
    relay(parts - 1)

    over_group(lambda d, p: gx(d, p, False).wait_recv())
    grecv[g] = gsend[g]

    def grad_sum(i, c):
        cols = pl.ds(pl.multiple_of(i * gch, gch), gch)
        grad_out[:, cols] = jnp.sum(grecv[:, :, cols].astype(F32), axis=0)
        return c
    lax.fori_loop(0, D // gch, grad_sum, 0)

    def drain_group(d, p):
        for x in (hx, tx, hzx, sx, gx):
            x(d, p, True).wait_send()
    over_group(drain_group)

    def drain_reps(d, p):
        for x in (zh, zx):
            x(d, p, True).wait_send()
        for k in range(parts):
            zw(k, d, p, True).wait_send()
    over_reps(drain_reps)
    for k in range(parts):
        for d in range(R):
            pl.when(jnp.logical_and(has_right, rep >= d))(lambda: nx(k, rep - d, 1).wait_send())
            pl.when(jnp.logical_and(has_left, rep + d < R))(lambda: nx(k, rep + d, -1).wait_send())


def flush(*refs):
    count = len(refs) // 2
    sems = refs[-1]
    copies = [pltpu.make_async_copy(refs[i], refs[count + i], sems.at[i]) for i in range(count)]
    for c in copies:
        c.start()
    for c in copies:
        c.wait()


def per_device(hidden, targets, unembed, outer_weight, momentum):
    R, T, V = lax.axis_size("rep"), lax.axis_size("tok"), lax.axis_size("voc")
    n = T * V
    _, rows, D = hidden.shape
    vocab = unembed.shape[1]
    slab, feat = outer_weight.shape
    tokens = n * rows
    lanes = -(-tokens // 128) * 128
    wch = min(256, vocab)
    gch = min(512, D)
    parts = 4 if slab % 128 == 0 else 1
    dma = pltpu.SemaphoreType.DMA
    vm = pltpu.VMEM
    spec_v = pl.BlockSpec(memory_space=pltpu.VMEM)
    spec_a = pl.BlockSpec(memory_space=pltpu.HBM)
    scratch = [
        vm((vocab, D), BF16), vm((n, rows, D), BF16), vm((tokens, D), BF16), vm((n, rows, 128), F32),
        vm((n, R, rows, feat), BF16), vm((R, slab, feat), BF16), vm((tokens, vocab), F32),
        vm((tokens, vocab), BF16), vm((R, tokens, slab), BF16), vm((n, 8, lanes), F32),
        vm((n, rows, D), BF16), vm((n, rows, D), BF16),
        vm((slab, feat), F32),
        dma((vocab // wch,)), dma((2,)),
        dma((n,)), dma((n,)), dma((n,)), dma((n,)), dma((R,)), dma((R,)), dma((parts, R)), dma((parts, R)),
        dma((n,)), dma((n,)), dma((n,)), dma((n,)), dma((R,)), dma((R,)), dma((n,)), dma((n,)),
        dma((parts, R)), dma((parts, R)), dma((parts, R)),
    ]
    results = pl.pallas_call(
        functools.partial(kernel, (R, T, V, rows, D, vocab, slab, feat, wch, gch, parts)),
        out_shape=(
            jax.ShapeDtypeStruct((1, rows), F32),
            jax.ShapeDtypeStruct((rows, D), F32),
            jax.ShapeDtypeStruct((slab, feat), F32),
            jax.ShapeDtypeStruct((slab, feat), F32),
            jax.ShapeDtypeStruct((slab, R * feat), BF16),
        ),
        in_specs=[spec_a, spec_v, spec_a, spec_v, spec_v],
        out_specs=(spec_v,) * 5,
        scratch_shapes=scratch,
        compiler_params=pltpu.CompilerParams(
            collective_id=0, has_side_effects=True, vmem_limit_bytes=50 * 2**20),
        name="step",
    )(hidden[0], targets, unembed[0], outer_weight, momentum)
    loss, grad, new_outer, new_mom, nxt = pl.pallas_call(
        flush,
        out_shape=tuple(jax.ShapeDtypeStruct(x.shape, x.dtype) for x in results),
        in_specs=[spec_v] * 5,
        out_specs=(spec_a,) * 5,
        scratch_shapes=[dma((5,))],
        compiler_params=pltpu.CompilerParams(vmem_limit_bytes=6 * 2**20),
        name="flush",
    )(*results)
    return (loss, grad[None], new_outer, new_mom, nxt)


def solution(mesh):
    group = ("tok", "voc")
    return jax.shard_map(
        per_device,
        mesh=mesh,
        in_specs=(P("rep", group, None), P("rep", group), P("rep", group, None), P(group, "rep"), P(group, "rep")),
        out_specs=(P("rep", group), P("rep", group, None), P(group, "rep"), P(group, "rep"), P(group, None)),
        check_vma=False,
    )
```

```python
import functools

import jax
import jax.numpy as jnp
from jax import lax
from jax.experimental import pallas as pl
from jax.experimental.pallas import tpu as pltpu
from jax.sharding import PartitionSpec as P

inner_rate = 0.5
outer_rate = 0.7
momentum_coef = 0.9
F32 = jnp.float32
BF16 = jnp.bfloat16


def kernel(
    sizes,
    hid, tgt, w_hbm, outer_v, mom_v,
    loss_out, grad_out, outer_out, mom_out, next_out,
    w, hbuf, h2d, tbuf, hz, wz, logits, errs, ez, stat, gsend, grecv, sgrad,
    wsem, lsem, hs, hr, ts, tr, zhs, zhr, zws, zwr, hzs, hzr, ss, sr, es, er, gs, gr, nright, nleft, nr,
):
    R, T, V, rows, D, vocab, slab, feat, wch, gch, parts = sizes
    prow = slab // parts
    n = T * V
    tokens = n * rows
    scale = D ** -0.5
    rep = lax.axis_index("rep")
    g = lax.axis_index("tok") * V + lax.axis_index("voc")

    def group_id(p):
        return {"tok": p // V, "voc": lax.rem(p, V)}

    def over_group(body):
        def step(d, c):
            body(d, lax.rem(g + d, n))
            return c
        lax.fori_loop(1, n, step, 0)

    def over_reps(body):
        for d in range(1, R):
            body(d, lax.rem(rep + d, R))

    def feats(p):
        return pl.ds(pl.multiple_of(p * feat, feat), feat)

    hid_in = pltpu.make_async_copy(hid, hbuf.at[g], lsem.at[0])
    hid_in.start()
    hz_in = pltpu.make_async_copy(hid.at[:, feats(rep)], hz.at[g, rep], lsem.at[1])
    hz_in.start()
    w_in = lambda c: pltpu.make_async_copy(
        w_hbm.at[pl.ds(pl.multiple_of(c * wch, wch), wch)],
        w.at[pl.ds(pl.multiple_of(c * wch, wch), wch)], wsem.at[c])
    for c in range(vocab // wch):
        w_in(c).start()

    diag = lax.broadcasted_iota(jnp.int32, (rows, rows), 0) == lax.broadcasted_iota(jnp.int32, (rows, rows), 1)
    trow = jnp.broadcast_to(tgt[...].astype(F32), (rows, rows))
    tcol = jnp.sum(jnp.where(diag, trow, 0.0), axis=1, keepdims=True)
    tbuf[g] = jnp.broadcast_to(tcol, (rows, 128))

    barrier = pltpu.get_barrier_semaphore()
    over_reps(lambda d, p: pl.semaphore_signal(barrier, inc=1, device_id={"rep": p}))
    over_group(lambda d, p: pl.semaphore_signal(barrier, inc=1, device_id=group_id(p)))
    pl.semaphore_wait(barrier, R - 1 + n - 1)

    def zh(d, p, s):
        return pltpu.make_async_remote_copy(
            hid.at[:, feats(p)], hz.at[g, rep if s else p], zhs.at[d], zhr.at[rep if s else p], device_id={"rep": p})

    def zw(k, d, p, s):
        o = rep if s else p
        return pltpu.make_async_remote_copy(
            w_hbm.at[pl.ds(k * prow, prow), feats(p)], wz.at[o, pl.ds(k * prow, prow)], zws.at[k, d], zwr.at[k, o],
            device_id={"rep": p})

    over_reps(lambda d, p: zh(d, p, True).start())
    hid_in.wait()

    def hx(d, p, s):
        o = g if s else p
        return pltpu.make_async_remote_copy(hbuf.at[g], hbuf.at[o], hs.at[d], hr.at[o], device_id=group_id(p))

    def tx(d, p, s):
        o = g if s else p
        return pltpu.make_async_remote_copy(tbuf.at[g], tbuf.at[o], ts.at[d], tr.at[o], device_id=group_id(p))

    def start_group(d, p):
        hx(d, p, True).start()
        tx(d, p, True).start()
    over_group(start_group)
    for k in range(max(parts - 1, 1)):
        over_reps(lambda d, p: zw(k, d, p, True).start())

    def wait_group(d, p):
        hx(d, p, False).wait_recv()
    over_group(wait_group)

    def pack(i, c):
        cols = pl.ds(pl.multiple_of(i * gch, gch), gch)
        h2d[:, cols] = hbuf[:, :, cols].astype(F32).reshape(tokens, gch).astype(BF16)
        return c
    lax.fori_loop(0, D // gch, pack, 0)

    def logit_step(c, carry):
        w_in(c).wait()
        at = pl.ds(pl.multiple_of(c * wch, wch), wch)
        logits[:, at] = lax.dot_general(
            h2d[...], w[at], (((1,), (1,)), ((), ())), preferred_element_type=F32) * scale
        return carry
    lax.fori_loop(0, vocab // wch, logit_step, 0)

    hz_in.wait()
    over_reps(lambda d, p: zh(d, p, False).wait_recv())

    def hzx(d, p, s):
        o = g if s else p
        return pltpu.make_async_remote_copy(hz.at[g], hz.at[o], hzs.at[d], hzr.at[o], device_id=group_id(p))

    over_group(lambda d, p: tx(d, p, False).wait_recv())
    l = logits[...]
    targets = tbuf[...].reshape(tokens, 128)[:, :1].astype(jnp.int32)
    onehot = targets == g * vocab + lax.broadcasted_iota(jnp.int32, (tokens, vocab), 1)
    top = jnp.max(l, axis=1, keepdims=True)
    ex = jnp.exp(l - top)
    total = jnp.sum(ex, axis=1, keepdims=True)
    tl = jnp.sum(jnp.where(onehot, l, 0.0), axis=1, keepdims=True)
    lanes = stat.shape[2]
    eye = lax.broadcasted_iota(jnp.int32, (tokens, lanes), 0) == lax.broadcasted_iota(jnp.int32, (tokens, lanes), 1)
    to_row = lambda col: jnp.sum(jnp.where(eye, col, 0.0), axis=0, keepdims=True)
    to_col = lambda row: jnp.sum(jnp.where(eye, row, 0.0), axis=1, keepdims=True)
    stat[g] = jnp.concatenate([to_row(top), to_row(total), to_row(tl), jnp.zeros((5, lanes), F32)], axis=0)

    def sx(d, p, s):
        o = g if s else p
        return pltpu.make_async_remote_copy(stat.at[g], stat.at[o], ss.at[d], sr.at[o], device_id=group_id(p))
    over_group(lambda d, p: sx(d, p, True).start())
    over_group(lambda d, p: hzx(d, p, True).start())
    over_group(lambda d, p: sx(d, p, False).wait_recv())
    st = stat[...]
    tops = st[:, 0:1, :]
    all_top = jnp.max(tops, axis=0)
    all_total = jnp.sum(st[:, 1:2, :] * jnp.exp(tops - all_top[None]), axis=0)
    log_total = all_top + jnp.log(all_total)
    loss_row = log_total - jnp.sum(st[:, 2:3, :], axis=0)
    loss_col = to_col(loss_row)
    mine = lax.broadcasted_iota(jnp.int32, (tokens, rows), 0) == g * rows + lax.broadcasted_iota(
        jnp.int32, (tokens, rows), 1)
    loss_out[...] = jnp.sum(jnp.where(mine, loss_col, 0.0), axis=0, keepdims=True)
    err = (jnp.exp(l - to_col(log_total)) - onehot.astype(F32)).astype(BF16)
    errs[...] = err
    ez[rep] = err[:, :slab]

    def zx(d, p, s):
        o = rep if s else p
        return pltpu.make_async_remote_copy(ez.at[rep], ez.at[o], es.at[d], er.at[o], device_id={"rep": p})
    over_reps(lambda d, p: zx(d, p, True).start())
    for k in range(1, parts)[-1:]:
        over_reps(lambda d, p: zw(k, d, p, True).start())

    def grad_step(i, c):
        cols = pl.ds(pl.multiple_of(i * gch, gch), gch)
        part = jnp.dot(errs[...], w[:, cols], preferred_element_type=F32) * scale
        gsend[:, :, cols] = part.reshape(n, rows, gch).astype(BF16)
        return c

    def gx(d, p, s):
        return pltpu.make_async_remote_copy(
            gsend.at[p], grecv.at[g if s else p], gs.at[d], gr.at[g if s else p], device_id=group_id(p))

    over_group(lambda d, p: hzx(d, p, False).wait_recv())
    over_reps(lambda d, p: zx(d, p, False).wait_recv())
    every_err = ez[...].astype(F32).reshape(R * tokens, slab).T.astype(BF16)
    every_hid = jnp.concatenate(
        [hz[:, r].astype(F32).reshape(tokens, feat).astype(BF16) for r in range(R)], axis=0)
    sgrad[...] = jnp.dot(every_err, every_hid, preferred_element_type=F32) * scale
    wz[rep] = w[:slab, feats(rep)]

    def nx(k, b, side):
        at = next_out.at[pl.ds(k * prow, prow), feats(b)]
        sems = nright if side > 0 else nleft
        return pltpu.make_async_remote_copy(
            at, at, sems.at[k, b], nr.at[k, b], device_id={"rep": lax.rem(rep + side + R, R)})

    has_right, has_left = rep < R - 1, rep > 0

    def outer_part(k):
        at = pl.ds(k * prow, prow)
        over_reps(lambda d, p: zw(k, d, p, False).wait_recv())
        final_sum = jnp.sum(wz[:, at].astype(F32), axis=0) - inner_rate * sgrad[at]
        outer = outer_v[at]
        pseudo = outer - final_sum / R
        moved_mom = momentum_coef * mom_v[at] + pseudo
        moved = outer - outer_rate * (pseudo + momentum_coef * moved_mom)
        mom_out[at] = moved_mom
        outer_out[at] = moved
        next_out[at, feats(rep)] = moved.astype(BF16)
        pl.when(has_right)(lambda: nx(k, rep, 1).start())
        pl.when(has_left)(lambda: nx(k, rep, -1).start())

    def relay(k):
        for d in range(1, R):
            @pl.when(rep >= d)
            def _():
                nx(k, rep - d, 1).wait_recv()
                pl.when(has_right)(lambda: nx(k, rep - d, 1).start())

            @pl.when(rep + d < R)
            def _():
                nx(k, rep + d, -1).wait_recv()
                pl.when(has_left)(lambda: nx(k, rep + d, -1).start())

    for k in range(max(parts - 1, 1)):
        outer_part(k)
    lax.fori_loop(0, D // gch, grad_step, 0)
    over_group(lambda d, p: gx(d, p, True).start())
    for k in range(1, parts)[-1:]:
        outer_part(k)
    for k in range(parts):
        relay(k)

    over_group(lambda d, p: gx(d, p, False).wait_recv())
    grecv[g] = gsend[g]

    def grad_sum(i, c):
        cols = pl.ds(pl.multiple_of(i * gch, gch), gch)
        grad_out[:, cols] = jnp.sum(grecv[:, :, cols].astype(F32), axis=0)
        return c
    lax.fori_loop(0, D // gch, grad_sum, 0)

    def drain_group(d, p):
        for x in (hx, tx, hzx, sx, gx):
            x(d, p, True).wait_send()
    over_group(drain_group)

    def drain_reps(d, p):
        for x in (zh, zx):
            x(d, p, True).wait_send()
        for k in range(parts):
            zw(k, d, p, True).wait_send()
    over_reps(drain_reps)
    for k in range(parts):
        for d in range(R):
            pl.when(jnp.logical_and(has_right, rep >= d))(lambda: nx(k, rep - d, 1).wait_send())
            pl.when(jnp.logical_and(has_left, rep + d < R))(lambda: nx(k, rep + d, -1).wait_send())


def flush(*refs):
    count = len(refs) // 2
    sems = refs[-1]
    copies = [pltpu.make_async_copy(refs[i], refs[count + i], sems.at[i]) for i in range(count)]
    for c in copies:
        c.start()
    for c in copies:
        c.wait()


def per_device(hidden, targets, unembed, outer_weight, momentum):
    R, T, V = lax.axis_size("rep"), lax.axis_size("tok"), lax.axis_size("voc")
    n = T * V
    _, rows, D = hidden.shape
    vocab = unembed.shape[1]
    slab, feat = outer_weight.shape
    tokens = n * rows
    lanes = -(-tokens // 128) * 128
    wch = min(256, vocab)
    gch = min(512, D)
    parts = 4 if slab % 128 == 0 else 1
    dma = pltpu.SemaphoreType.DMA
    vm = pltpu.VMEM
    spec_v = pl.BlockSpec(memory_space=pltpu.VMEM)
    spec_a = pl.BlockSpec(memory_space=pltpu.HBM)
    scratch = [
        vm((vocab, D), BF16), vm((n, rows, D), BF16), vm((tokens, D), BF16), vm((n, rows, 128), F32),
        vm((n, R, rows, feat), BF16), vm((R, slab, feat), BF16), vm((tokens, vocab), F32),
        vm((tokens, vocab), BF16), vm((R, tokens, slab), BF16), vm((n, 8, lanes), F32),
        vm((n, rows, D), BF16), vm((n, rows, D), BF16),
        vm((slab, feat), F32),
        dma((vocab // wch,)), dma((2,)),
        dma((n,)), dma((n,)), dma((n,)), dma((n,)), dma((R,)), dma((R,)), dma((parts, R)), dma((parts, R)),
        dma((n,)), dma((n,)), dma((n,)), dma((n,)), dma((R,)), dma((R,)), dma((n,)), dma((n,)),
        dma((parts, R)), dma((parts, R)), dma((parts, R)),
    ]
    results = pl.pallas_call(
        functools.partial(kernel, (R, T, V, rows, D, vocab, slab, feat, wch, gch, parts)),
        out_shape=(
            jax.ShapeDtypeStruct((1, rows), F32),
            jax.ShapeDtypeStruct((rows, D), F32),
            jax.ShapeDtypeStruct((slab, feat), F32),
            jax.ShapeDtypeStruct((slab, feat), F32),
            jax.ShapeDtypeStruct((slab, R * feat), BF16),
        ),
        in_specs=[spec_a, spec_v, spec_a, spec_v, spec_v],
        out_specs=(spec_v,) * 5,
        scratch_shapes=scratch,
        compiler_params=pltpu.CompilerParams(
            collective_id=0, has_side_effects=True, vmem_limit_bytes=50 * 2**20),
        name="step",
    )(hidden[0], targets, unembed[0], outer_weight, momentum)
    loss, grad, new_outer, new_mom, nxt = pl.pallas_call(
        flush,
        out_shape=tuple(jax.ShapeDtypeStruct(x.shape, x.dtype) for x in results),
        in_specs=[spec_v] * 5,
        out_specs=(spec_a,) * 5,
        scratch_shapes=[dma((5,))],
        compiler_params=pltpu.CompilerParams(vmem_limit_bytes=6 * 2**20),
        name="flush",
    )(*results)
    return (loss, grad[None], new_outer, new_mom, nxt)


def solution(mesh):
    group = ("tok", "voc")
    return jax.shard_map(
        per_device,
        mesh=mesh,
        in_specs=(P("rep", group, None), P("rep", group), P("rep", group, None), P(group, "rep"), P(group, "rep")),
        out_specs=(P("rep", group), P("rep", group, None), P(group, "rep"), P(group, "rep"), P(group, None)),
        check_vma=False,
    )
```
